32 devices in a mesh: dp: 16 (over z, y, core), tensor: 2 (over x).
Axes of the slice: x: 2, y: 2, z: 4, core: 2. Of those that a mesh axis runs over, the one named last changes fastest.
Arguments:
- token_ids: int32 [8192], P('dp'), may hold values from 0 to 30719
- lengths: int32 [16], P('dp'), may hold values from 128 to 512
- word_table: bfloat16 [30720, 1024], P('tensor'), may hold values from -6 to 6
- pos_table: bfloat16 [512, 1024], replicated, may hold values from -4 to 4
- w_qkv: bfloat16 [2, 3, 1024, 1024], P(None, None, 'dp', 'tensor'), may hold values from -0.1875 to 0.1875
- w_out: bfloat16 [2, 1024, 1024], P(None, 'dp', 'tensor'), may hold values from -0.1875 to 0.1875
- w_up: bfloat16 [2, 1024, 4096], P(None, 'dp', 'tensor'), may hold values from -0.1875 to 0.1875
- w_down: bfloat16 [2, 1024, 4096], P(None, 'dp', 'tensor'), may hold values from -0.09375 to 0.09375
- up_bias: float32 [2, 4096], P(None, 'tensor'), may hold values from -3 to 3
- dense_bias: float32 [2, 2, 1024], replicated, may hold values from -3 to 3
- norm_gain: float32 [5, 1024], replicated, may hold values from 0.1 to 1.9
- norm_bias: float32 [5, 1024], replicated, may hold values from -3 to 3
Outputs:
- encoded: bfloat16 [8192, 1024], P('dp', 'tensor')
- similarity: float32 [16, 16], P('dp')
The draws below stay inside these ranges and needn't reach their ends.
All inputs are finite; a program needn't handle non-finite values.
Results may differ from the reference program's by a relative error of at most 0.015.
Values may be sent and summed in bfloat16 or wider, within the bound.
A program may use at most 128 MiB of HBM per device.

```python
import math
import jax
import jax.numpy as jnp
import numpy as np
from jax import lax

D = 1024
HEADS = 16
FF = 4096
VOCAB = 30720
BLOCK = 512
LAYERS = 2
HEAD = 64
BLOCKS = 16
TOKENS = 8192
N_TENSOR = 2


def with_ends(entries, stream_key, smallest, high):
    shape = entries.shape
    spot = [jax.random.randint(jax.random.fold_in(stream_key, axis), (), 0, shape[axis]) for axis in range(len(shape))]
    entries = entries.at[tuple(spot)].set(smallest)
    longest = shape.index(max(shape))
    spot[longest] = (spot[longest] + 1) % shape[longest]
    return entries.at[tuple(spot)].set(high)


def levels(rng, extent, split, least, top_value):
    factor_of = 1.0
    for axis_at, shards_of in split:
        steps = jax.random.uniform(jax.random.fold_in(jax.random.fold_in(rng, 6), axis_at), (shards_of,), jnp.float32, least / len(split), top_value / len(split))
        factor_of = factor_of * jnp.repeat(jnp.exp(steps), extent[axis_at] // shards_of).reshape((-1,) + (1,) * (len(extent) - 1 - axis_at))
    return factor_of


def rank_bounds(number_of, slope):
    loads = [(1 << 20) // math.isqrt(rank ** slope) + 1 for rank in range(1, number_of + 1)]
    scale = 1 + sum(loads) // (1 << 30)
    return np.cumsum(np.array([max(1, weight // scale) for weight in loads]))


def skewed_ids(own_key, extent, amount, slope):
    table = rank_bounds(amount, slope)
    ticket = jax.random.randint(jax.random.fold_in(own_key, 1), extent, 0, int(table[amount - 1]))
    grade = jnp.searchsorted(jnp.asarray(table, jnp.int32), ticket, side="right")
    return jax.random.permutation(jax.random.fold_in(own_key, 2), amount)[grade].astype(jnp.int32)


def noise(key, extent, scale, reach, pieces=(), kind=jnp.bfloat16):
    level = levels(key, extent, pieces, -0.22, 0.18) if pieces else 1.0
    array = jax.random.normal(key, extent, jnp.float32) * scale * level
    return jnp.minimum(jnp.maximum(array, -reach), reach).astype(kind)


def setup_inputs(seed: int = 0) -> dict:
    key_list = jax.random.split(jax.random.key(seed), 13)
    token_ids = with_ends(skewed_ids(key_list[0], (TOKENS,), VOCAB, 2), jax.random.fold_in(key_list[0], 3), 0, VOCAB - 1).astype(jnp.int32)
    lengths = with_ends(jax.random.randint(key_list[1], (BLOCKS,), BLOCK // 4, BLOCK + 1), jax.random.fold_in(key_list[1], 1), BLOCK // 4, BLOCK).astype(jnp.int32)
    word_table = noise(key_list[2], (VOCAB, D), 1.0, 6.0, ((0, 2),))
    pos_table = noise(key_list[3], (BLOCK, D), 0.5, 4.0)
    w_qkv = noise(key_list[4], (LAYERS, 3, D, D), D ** -0.5, 0.1875, ((2, 16), (3, 2)))
    w_out = noise(key_list[5], (LAYERS, D, D), D ** -0.5, 0.1875, ((1, 16), (2, 2)))
    w_up = noise(key_list[6], (LAYERS, D, FF), D ** -0.5, 0.1875, ((1, 16), (2, 2)))
    w_down = noise(key_list[7], (LAYERS, D, FF), FF ** -0.5, 0.09375, ((1, 16), (2, 2)))
    up_bias = noise(key_list[8], (LAYERS, FF), 0.5, 3.0, ((1, 2),), jnp.float32)
    dense_bias = noise(key_list[9], (LAYERS, 2, D), 0.5, 3.0, (), jnp.float32)
    norm_gain = jnp.clip(1.0 + 0.18 * jax.random.normal(key_list[10], (2 * LAYERS + 1, D), jnp.float32), 0.1, 1.9)
    norm_bias = noise(key_list[11], (2 * LAYERS + 1, D), 0.5, 3.0, (), jnp.float32)
    return {"token_ids": token_ids, "lengths": lengths, "word_table": word_table, "pos_table": pos_table, "w_qkv": w_qkv, "w_out": w_out, "w_up": w_up, "w_down": w_down, "up_bias": up_bias, "dense_bias": dense_bias, "norm_gain": norm_gain, "norm_bias": norm_bias}


EPS = 1e-05

def layer_norm(values, gain, shift):
    average = lax.optimization_barrier(jnp.mean(values, axis=-1, keepdims=True))
    centered = values - average
    spread = lax.optimization_barrier(jnp.mean(centered * centered, axis=-1, keepdims=True))
    return centered * lax.rsqrt(spread + EPS) * gain + shift

def group_sum(left, weight, width):
    groups = left.shape[1] // width
    left_g = left.reshape(left.shape[0], groups, width).astype(jnp.float32)
    right_g = weight.reshape(weight.shape[0], groups, width).astype(jnp.float32)
    partial_value = jnp.einsum('tgc,dgc->gtd', left_g, right_g)
    return lax.optimization_barrier(jnp.sum(partial_value.astype(jnp.bfloat16).astype(jnp.float32), axis=0))

def reference(token_ids, lengths, word_table, pos_table, w_qkv, w_out, w_up, w_down, up_bias, dense_bias, norm_gain, norm_bias):

    def encode(args):
        passage_ids, length = args
        embedded = word_table[passage_ids].astype(jnp.float32) + pos_table.astype(jnp.float32)
        hidden = layer_norm(embedded, norm_gain[0], norm_bias[0]).astype(jnp.bfloat16)
        visible = jnp.arange(BLOCK, dtype=jnp.int32) < length
        for layer in range(LAYERS):
            projected = jnp.einsum('td,idc->itc', hidden.astype(jnp.float32), w_qkv[layer].astype(jnp.float32)).astype(jnp.bfloat16)
            query = projected[0].reshape(BLOCK, HEADS, HEAD).astype(jnp.float32)
            keys = projected[1].reshape(BLOCK, HEADS, HEAD).astype(jnp.float32)
            values = projected[2].reshape(BLOCK, HEADS, HEAD).astype(jnp.float32)
            scores = jnp.einsum('qhe,khe->hqk', query, keys) / jnp.sqrt(jnp.float32(HEAD))
            scores = jnp.where(visible[None, None, :], scores, jnp.float32(-1e+30))
            top = lax.optimization_barrier(jnp.max(scores, axis=-1, keepdims=True))
            expo = jnp.exp(scores - top)
            weights_soft = (expo / lax.optimization_barrier(jnp.sum(expo, axis=-1, keepdims=True))).astype(jnp.bfloat16)
            context = jnp.einsum('hqk,khe->qhe', weights_soft.astype(jnp.float32), values).astype(jnp.bfloat16).reshape(BLOCK, D)
            attended = group_sum(context, w_out[layer], D // N_TENSOR)
            middle = layer_norm(hidden.astype(jnp.float32) + attended + dense_bias[layer, 0], norm_gain[2 * layer + 1], norm_bias[2 * layer + 1]).astype(jnp.bfloat16)
            inner = jax.nn.gelu(jnp.dot(middle, w_up[layer], preferred_element_type=jnp.float32) + up_bias[layer], approximate=False).astype(jnp.bfloat16)
            mlp_out = group_sum(inner, w_down[layer], FF // N_TENSOR)
            hidden = layer_norm(middle.astype(jnp.float32) + mlp_out + dense_bias[layer, 1], norm_gain[2 * layer + 2], norm_bias[2 * layer + 2]).astype(jnp.bfloat16)
        weights_pool = visible.astype(jnp.float32)
        pooled = lax.optimization_barrier(jnp.sum(weights_pool[:, None] * hidden.astype(jnp.float32), axis=0)) / length.astype(jnp.float32)
        unit = pooled * lax.rsqrt(jnp.sum(pooled * pooled) + 1e-06)
        return (hidden, unit)
    states, units = lax.map(encode, (token_ids.reshape(BLOCKS, BLOCK), lengths))
    encoded = states.reshape(TOKENS, D)
    similarity = jnp.dot(units, units.T, precision=lax.Precision.HIGHEST, preferred_element_type=jnp.float32)
    return (encoded, similarity)
```

```python
import functools

import jax
import jax.numpy as jnp
from jax import lax
from jax.experimental import pallas as pl
from jax.experimental.pallas import tpu as pltpu
from jax.sharding import PartitionSpec as P

D = 1024
BLOCK = 512
LAYERS = 2
HEAD = 64


EPS = 1e-05


def layer_norm(values, gain, shift):
    average = jnp.mean(values, axis=-1, keepdims=True)
    centered = values - average
    spread = jnp.mean(centered * centered, axis=-1, keepdims=True)
    return centered * lax.rsqrt(spread + EPS) * gain + shift


def swap_sum(part):
    n = lax.axis_size("tensor")
    total = part.astype(jnp.float32)
    for shift in range(1, n):
        total = total + lax.ppermute(
            part, "tensor", [(i, (i + shift) % n) for i in range(n)]
        ).astype(jnp.float32)
    return total


def settle(part, residual, bias_row, gain, shift):
    summed = swap_sum(part)
    return layer_norm(residual.astype(jnp.float32) + summed + bias_row, gain, shift).astype(
        jnp.bfloat16
    )


def stages(n):
    if n % 4 == 0:
        return [n // 4, 2, 2]
    return [n]


def gather_dp(shard):
    n = lax.axis_size("dp")
    sizes = stages(n)
    me = lax.axis_index("dp")
    held = shard.reshape(shard.shape[0], 1, *shard.shape[1:])
    stride = n
    for size in sizes:
        stride //= size
        digit = lax.rem(me // stride, size)
        k, m, rows, cols = held.shape
        whole = jnp.zeros((k, m, size, rows, cols), held.dtype)
        for shift in range(size):
            if shift == 0:
                block = held
            else:
                moves = []
                for i in range(n):
                    d = (i // stride) % size
                    moves.append((i, i + ((d + shift) % size - d) * stride))
                block = lax.ppermute(held, "dp", moves)
            source = lax.rem(digit - shift + size, size)
            whole = lax.dynamic_update_slice(
                whole, block[:, :, None], (0, 0, source, 0, 0)
            )
        held = whole.reshape(k, m * size, rows, cols)
    k, m, rows, cols = held.shape
    return held.reshape(k, m * rows, cols)


def share_kernel(n, unit_ref, every_ref, held, send_sem, recv_sem):
    me = lax.axis_index("dp")
    barrier = pltpu.get_barrier_semaphore()
    for shift in range(1, n):
        pl.semaphore_signal(
            barrier,
            inc=1,
            device_id={"dp": lax.rem(me + shift, n)},
            device_id_type=pl.DeviceIdType.MESH,
        )
    pl.semaphore_wait(barrier, n - 1)
    copies = []
    for shift in range(1, n):
        copy = pltpu.make_async_remote_copy(
            src_ref=unit_ref,
            dst_ref=held.at[shift],
            send_sem=send_sem.at[shift],
            recv_sem=recv_sem.at[shift],
            device_id={"dp": lax.rem(me + shift, n)},
            device_id_type=pl.DeviceIdType.MESH,
        )
        copy.start()
        copies.append(copy)
    every_ref[me] = unit_ref[...]
    for shift in range(1, n):
        copies[shift - 1].wait()
        every_ref[lax.rem(me - shift + n, n)] = held[shift]


def share_units(unit):
    n = lax.axis_size("dp")
    passages, width = unit.shape
    tile = unit.reshape(passages * width // 128, 128)
    every = pl.pallas_call(
        functools.partial(share_kernel, n),
        out_shape=jax.ShapeDtypeStruct((n, *tile.shape), tile.dtype),
        in_specs=[pl.BlockSpec(memory_space=pltpu.VMEM)],
        out_specs=pl.BlockSpec(memory_space=pltpu.VMEM),
        scratch_shapes=[
            pltpu.VMEM((n, *tile.shape), tile.dtype),
            pltpu.SemaphoreType.DMA((n,)),
            pltpu.SemaphoreType.DMA((n,)),
        ],
        compiler_params=pltpu.CompilerParams(collective_id=0, has_side_effects=True),
    )(tile)
    return every.reshape(n * passages, width)


def project_back(left, weight):
    product = lax.dot_general(
        left, weight, (((1,), (1,)), ((), ())), preferred_element_type=jnp.float32
    )
    return product.astype(jnp.bfloat16)


def per_device(
    token_ids,
    lengths,
    word_table,
    pos_table,
    w_qkv,
    w_out,
    w_up,
    w_down,
    up_bias,
    dense_bias,
    norm_gain,
    norm_bias,
):
    passage_count = lengths.shape[0]
    vocab_rows = word_table.shape[0]
    local_ids = token_ids - lax.axis_index("tensor") * vocab_rows
    inside = (local_ids >= 0) & (local_ids < vocab_rows)
    picked = jnp.take(word_table, jnp.clip(local_ids, 0, vocab_rows - 1), axis=0)
    picked = jnp.where(inside[:, None], picked, jnp.zeros_like(picked))
    embedded = swap_sum(picked)
    embedded = embedded.reshape(passage_count, BLOCK, D) + pos_table.astype(jnp.float32)[None]
    hidden = layer_norm(
        embedded.reshape(passage_count * BLOCK, D), norm_gain[0], norm_bias[0]
    ).astype(jnp.bfloat16)
    visible = jnp.arange(BLOCK, dtype=jnp.int32)[None, :] < lengths[:, None]
    local_heads = w_qkv.shape[3] // HEAD
    scale_dot = 1.0 / jnp.sqrt(jnp.float32(HEAD))
    gathered = []
    for layer in range(LAYERS):
        gathered.append(
            (
                gather_dp(jnp.concatenate([w_qkv[layer], w_out[layer][None]], axis=0)),
                gather_dp(jnp.stack([w_up[layer], w_down[layer]], axis=0)),
            )
        )
    for layer in range(LAYERS):
        mixers, mlps = gathered[layer]
        columns = hidden
        projected = jnp.einsum(
            "td,idc->itc",
            columns,
            mixers[:3],
            preferred_element_type=jnp.float32,
        )
        projected = projected.astype(jnp.bfloat16).reshape(
            3, passage_count, BLOCK, local_heads, HEAD
        )
        scores = (
            jnp.einsum(
                "cqhe,ckhe->chqk", projected[0], projected[1], preferred_element_type=jnp.float32
            )
            * scale_dot
        )
        scores = jnp.where(visible[:, None, None, :], scores, jnp.float32(-1e30))
        top = jnp.max(scores, axis=-1, keepdims=True)
        expo = jnp.exp(scores - top)
        weights_soft = (expo / jnp.sum(expo, axis=-1, keepdims=True)).astype(jnp.bfloat16)
        context = jnp.einsum(
            "chqk,ckhe->cqhe", weights_soft, projected[2], preferred_element_type=jnp.float32
        )
        context = context.astype(jnp.bfloat16).reshape(passage_count * BLOCK, local_heads * HEAD)
        attended = project_back(context, mixers[3])
        middle = settle(
            attended,
            hidden,
            dense_bias[layer, 0],
            norm_gain[2 * layer + 1],
            norm_bias[2 * layer + 1],
        )
        raised = jnp.dot(
            middle,
            mlps[0],
            preferred_element_type=jnp.float32,
        )
        inner = jax.nn.gelu(raised + up_bias[layer], approximate=False).astype(jnp.bfloat16)
        mlp_out = project_back(inner, mlps[1])
        hidden = settle(
            mlp_out,
            middle,
            dense_bias[layer, 1],
            norm_gain[2 * layer + 2],
            norm_bias[2 * layer + 2],
        )
    width_share = hidden.shape[1] // lax.axis_size("tensor")
    encoded = lax.dynamic_slice_in_dim(
        hidden, lax.axis_index("tensor") * width_share, width_share, 1
    )
    weights_pool = visible.astype(jnp.float32)
    states = hidden.reshape(passage_count, BLOCK, D).astype(jnp.float32)
    pooled = (
        jnp.sum(weights_pool[:, :, None] * states, axis=1) / lengths.astype(jnp.float32)[:, None]
    )
    unit = pooled * lax.rsqrt(jnp.sum(pooled * pooled, axis=1, keepdims=True) + 1e-06)
    every_unit = share_units(unit)
    similarity = jnp.dot(
        unit, every_unit.T, precision=lax.Precision.HIGHEST, preferred_element_type=jnp.float32
    )
    return (encoded, similarity)


def solution(mesh):
    in_specs = (
        P("dp"),
        P("dp"),
        P("tensor", None),
        P(),
        P(None, None, "dp", "tensor"),
        P(None, "dp", "tensor"),
        P(None, "dp", "tensor"),
        P(None, "dp", "tensor"),
        P(None, "tensor"),
        P(),
        P(),
        P(),
    )
    out_specs = (P("dp", "tensor"), P("dp", None))
    return jax.shard_map(
        per_device, mesh=mesh, in_specs=in_specs, out_specs=out_specs, check_vma=False
    )
```

```python
import functools

import jax
import jax.numpy as jnp
from jax import lax
from jax.experimental import pallas as pl
from jax.experimental.pallas import tpu as pltpu
from jax.sharding import PartitionSpec as P

D = 1024
BLOCK = 512
LAYERS = 2
HEAD = 64


EPS = 1e-05


def layer_norm(values, gain, shift):
    average = jnp.mean(values, axis=-1, keepdims=True)
    centered = values - average
    spread = jnp.mean(centered * centered, axis=-1, keepdims=True)
    return centered * lax.rsqrt(spread + EPS) * gain + shift


def swap(part):
    n = lax.axis_size("tensor")
    return [
        lax.ppermute(part, "tensor", [(i, (i + shift) % n) for i in range(n)])
        for shift in range(1, n)
    ]


def settle(part, residual, bias_row, gain, shift, others):
    summed = part.astype(jnp.float32)
    for other in others:
        summed = summed + other.astype(jnp.float32)
    return layer_norm(residual.astype(jnp.float32) + summed + bias_row, gain, shift).astype(
        jnp.bfloat16
    )


def digits_of(n):
    if n % 4 == 0:
        return n // 4, 2, 2
    return n, 1, 1


def link_kernel(n, peers, layer, count, part_ref, *refs):
    shards = [ref.at[layer] for ref in refs[:count]]
    others_ref = refs[count]
    wholes = refs[count + 1 : 2 * count + 1]
    send_sem, recv_sem, part_send, part_recv = refs[2 * count + 1 :]
    far, near, cores = digits_of(n)
    me = lax.axis_index("dp")
    rank = lax.axis_index("tensor")
    z, y, c = me // (near * cores), lax.rem(me // cores, near), lax.rem(me, cores)

    def index(dz, dy, dc):
        return (
            lax.rem(z + dz + far, far) * near + lax.rem(y + dy + near, near)
        ) * cores + lax.rem(c + dc + cores, cores)

    def peer(shift):
        return {"tensor": lax.rem(rank + shift, peers)}

    targets = [{"dp": index(dz, 0, 0)} for dz in range(1, far)]
    targets += [{"dp": index(0, dy, 0)} for dy in range(1, near)]
    targets += [{"dp": index(0, 0, dc)} for dc in range(1, cores)]
    targets += [peer(shift) for shift in range(1, peers)]
    barrier = pltpu.get_barrier_semaphore()
    for target in targets:
        pl.semaphore_signal(
            barrier, inc=1, device_id=target, device_id_type=pl.DeviceIdType.MESH
        )
    pl.semaphore_wait(barrier, len(targets))

    def slot(w, i):
        whole = wholes[w]
        return whole.at[:, i] if len(whole.shape) == 4 else whole.at[i]

    copies = {}

    def send(w, source, owner, target, dz, dy, dc):
        sem = ((w * far + dz) * near + dy) * cores + dc
        copy = pltpu.make_async_remote_copy(
            src_ref=source,
            dst_ref=slot(w, owner),
            send_sem=send_sem.at[sem],
            recv_sem=recv_sem.at[sem],
            device_id={"dp": target},
            device_id_type=pl.DeviceIdType.MESH,
        )
        copy.start()
        copies[w, dz, dy, dc] = copy

    swaps = []
    for shift in range(1, peers):
        swapped = pltpu.make_async_remote_copy(
            src_ref=part_ref,
            dst_ref=others_ref.at[shift - 1],
            send_sem=part_send.at[shift - 1],
            recv_sem=part_recv.at[shift - 1],
            device_id=peer(shift),
            device_id_type=pl.DeviceIdType.MESH,
        )
        swapped.start()
        swaps.append(swapped)
    for w in range(count):
        if far > 1:
            send(w, shards[w], me, index(1, 0, 0), 1, 0, 0)
        for dy in range(1, near):
            send(w, shards[w], me, index(0, dy, 0), 0, dy, 0)
        for dc in range(1, cores):
            send(w, shards[w], me, index(0, 0, dc), 0, 0, dc)
    for w in range(count):
        slot(w, me)[...] = shards[w][...]
    for dz in range(1, far):
        for w in range(count):
            copies[w, dz, 0, 0].wait_recv()
            owner = index(-dz, 0, 0)
            if dz + 1 < far:
                send(w, slot(w, owner), owner, index(1, 0, 0), dz + 1, 0, 0)
            for dy in range(1, near):
                send(w, slot(w, owner), owner, index(0, dy, 0), dz, dy, 0)
            for dc in range(1, cores):
                send(w, slot(w, owner), owner, index(0, 0, dc), dz, 0, dc)
    for dz in range(far):
        for dy in range(1, near):
            for w in range(count):
                copies[w, dz, dy, 0].wait_recv()
                owner = index(-dz, -dy, 0)
                for dc in range(1, cores):
                    send(w, slot(w, owner), owner, index(0, 0, dc), dz, dy, dc)
    for w in range(count):
        for dc in range(1, cores):
            for dz in range(far):
                for dy in range(near):
                    copies[w, dz, dy, dc].wait_recv()
    for copy in copies.values():
        copy.wait_send()
    for swapped in swaps:
        swapped.wait()


def link(part, layer, shards, ident):
    n, peers = lax.axis_size("dp"), lax.axis_size("tensor")
    vmem = pl.BlockSpec(memory_space=pltpu.VMEM)
    shapes = [jax.ShapeDtypeStruct((peers - 1, *part.shape), part.dtype)]
    for shard in shards:
        lead, (rows, cols) = shard.shape[1:-2], shard.shape[-2:]
        shapes.append(jax.ShapeDtypeStruct((*lead, n, rows, cols), shard.dtype))
    others, *wholes = pl.pallas_call(
        functools.partial(link_kernel, n, peers, layer, len(shards)),
        out_shape=shapes,
        in_specs=[vmem] * (1 + len(shards)),
        out_specs=[vmem] * len(shapes),
        scratch_shapes=[
            pltpu.SemaphoreType.DMA((len(shards) * n,)),
            pltpu.SemaphoreType.DMA((len(shards) * n,)),
            pltpu.SemaphoreType.DMA((peers - 1,)),
            pltpu.SemaphoreType.DMA((peers - 1,)),
        ],
        compiler_params=pltpu.CompilerParams(collective_id=ident, has_side_effects=True),
    )(part, *shards)
    joined = [
        whole.reshape(*whole.shape[:-3], whole.shape[-3] * whole.shape[-2], whole.shape[-1])
        for whole in wholes
    ]
    return list(others), joined


def share_kernel(n, unit_ref, every_ref, held, send_sem, recv_sem):
    me = lax.axis_index("dp")
    barrier = pltpu.get_barrier_semaphore()
    for shift in range(1, n):
        pl.semaphore_signal(
            barrier,
            inc=1,
            device_id={"dp": lax.rem(me + shift, n)},
            device_id_type=pl.DeviceIdType.MESH,
        )
    pl.semaphore_wait(barrier, n - 1)
    copies = []
    for shift in range(1, n):
        copy = pltpu.make_async_remote_copy(
            src_ref=unit_ref,
            dst_ref=held.at[shift],
            send_sem=send_sem.at[shift],
            recv_sem=recv_sem.at[shift],
            device_id={"dp": lax.rem(me + shift, n)},
            device_id_type=pl.DeviceIdType.MESH,
        )
        copy.start()
        copies.append(copy)
    every_ref[me] = unit_ref[...]
    for shift in range(1, n):
        copies[shift - 1].wait()
        every_ref[lax.rem(me - shift + n, n)] = held[shift]


def share_units(unit):
    n = lax.axis_size("dp")
    passages, width = unit.shape
    tile = unit.reshape(passages * width // 128, 128)
    every = pl.pallas_call(
        functools.partial(share_kernel, n),
        out_shape=jax.ShapeDtypeStruct((n, *tile.shape), tile.dtype),
        in_specs=[pl.BlockSpec(memory_space=pltpu.VMEM)],
        out_specs=pl.BlockSpec(memory_space=pltpu.VMEM),
        scratch_shapes=[
            pltpu.VMEM((n, *tile.shape), tile.dtype),
            pltpu.SemaphoreType.DMA((n,)),
            pltpu.SemaphoreType.DMA((n,)),
        ],
        compiler_params=pltpu.CompilerParams(collective_id=0, has_side_effects=True),
    )(tile)
    return every.reshape(n * passages, width)


def project_back(left, weight):
    product = lax.dot_general(
        left, weight, (((1,), (1,)), ((), ())), preferred_element_type=jnp.float32
    )
    return product.astype(jnp.bfloat16)


def per_device(
    token_ids,
    lengths,
    word_table,
    pos_table,
    w_qkv,
    w_out,
    w_up,
    w_down,
    up_bias,
    dense_bias,
    norm_gain,
    norm_bias,
):
    passage_count = lengths.shape[0]
    vocab_rows = word_table.shape[0]
    local_ids = token_ids - lax.axis_index("tensor") * vocab_rows
    inside = (local_ids >= 0) & (local_ids < vocab_rows)
    picked = jnp.take(word_table, jnp.clip(local_ids, 0, vocab_rows - 1), axis=0)
    picked = jnp.where(inside[:, None], picked, jnp.zeros_like(picked))
    others, (whole_qkv, whole_out) = link(picked, 0, [w_qkv, w_out], 1)
    embedded = picked.astype(jnp.float32)
    for other in others:
        embedded = embedded + other.astype(jnp.float32)
    embedded = embedded.reshape(passage_count, BLOCK, D) + pos_table.astype(jnp.float32)[None]
    hidden = layer_norm(
        embedded.reshape(passage_count * BLOCK, D), norm_gain[0], norm_bias[0]
    ).astype(jnp.bfloat16)
    visible = jnp.arange(BLOCK, dtype=jnp.int32)[None, :] < lengths[:, None]
    local_heads = w_qkv.shape[3] // HEAD
    scale_dot = 1.0 / jnp.sqrt(jnp.float32(HEAD))
    for layer in range(LAYERS):
        columns = hidden
        projected = jnp.einsum(
            "td,idc->itc",
            columns,
            whole_qkv,
            preferred_element_type=jnp.float32,
        )
        projected = projected.astype(jnp.bfloat16).reshape(
            3, passage_count, BLOCK, local_heads, HEAD
        )
        scores = (
            jnp.einsum(
                "cqhe,ckhe->chqk", projected[0], projected[1], preferred_element_type=jnp.float32
            )
            * scale_dot
        )
        scores = jnp.where(visible[:, None, None, :], scores, jnp.float32(-1e30))
        top = jnp.max(scores, axis=-1, keepdims=True)
        expo = jnp.exp(scores - top)
        weights_soft = (expo / jnp.sum(expo, axis=-1, keepdims=True)).astype(jnp.bfloat16)
        context = jnp.einsum(
            "chqk,ckhe->cqhe", weights_soft, projected[2], preferred_element_type=jnp.float32
        )
        context = context.astype(jnp.bfloat16).reshape(passage_count * BLOCK, local_heads * HEAD)
        attended = project_back(context, whole_out)
        others, (whole_up, whole_down) = link(attended, layer, [w_up, w_down], 2 * layer + 2)
        middle = settle(
            attended,
            hidden,
            dense_bias[layer, 0],
            norm_gain[2 * layer + 1],
            norm_bias[2 * layer + 1],
            others,
        )
        raised = jnp.dot(
            middle,
            whole_up,
            preferred_element_type=jnp.float32,
        )
        inner = jax.nn.gelu(raised + up_bias[layer], approximate=False).astype(jnp.bfloat16)
        mlp_out = project_back(inner, whole_down)
        if layer + 1 < LAYERS:
            others, (whole_qkv, whole_out) = link(
                mlp_out, layer + 1, [w_qkv, w_out], 2 * layer + 3
            )
        else:
            others = swap(mlp_out)
        hidden = settle(
            mlp_out,
            middle,
            dense_bias[layer, 1],
            norm_gain[2 * layer + 2],
            norm_bias[2 * layer + 2],
            others,
        )
    width_share = hidden.shape[1] // lax.axis_size("tensor")
    encoded = lax.dynamic_slice_in_dim(
        hidden, lax.axis_index("tensor") * width_share, width_share, 1
    )
    weights_pool = visible.astype(jnp.float32)
    states = hidden.reshape(passage_count, BLOCK, D).astype(jnp.float32)
    pooled = (
        jnp.sum(weights_pool[:, :, None] * states, axis=1) / lengths.astype(jnp.float32)[:, None]
    )
    unit = pooled * lax.rsqrt(jnp.sum(pooled * pooled, axis=1, keepdims=True) + 1e-06)
    every_unit = share_units(unit)
    similarity = jnp.dot(
        unit, every_unit.T, precision=lax.Precision.HIGHEST, preferred_element_type=jnp.float32
    )
    return (encoded, similarity)


def solution(mesh):
    in_specs = (
        P("dp"),
        P("dp"),
        P("tensor", None),
        P(),
        P(None, None, "dp", "tensor"),
        P(None, "dp", "tensor"),
        P(None, "dp", "tensor"),
        P(None, "dp", "tensor"),
        P(None, "tensor"),
        P(),
        P(),
        P(),
    )
    out_specs = (P("dp", "tensor"), P("dp", None))
    return jax.shard_map(
        per_device, mesh=mesh, in_specs=in_specs, out_specs=out_specs, check_vma=False
    )
```
